32 devices in a mesh: dp: 4 (over z), feat: 8 (over y, x, core).
Axes of the slice: x: 2, y: 2, z: 4, core: 2. Of those that a mesh axis runs over, the one named last changes fastest.
Arguments:
- features: float32 [4096, 8192], P('dp', 'feat'), may hold values from -0.0625 to 0.0625
- labels: int32 [4096], P('dp'), may hold values from -1 to 1, as said below
- weights: float32 [8192], P('feat'), may hold values from -6 to 6
Outputs:
- gradient: float32 [8192], P('feat')
- newton_step: float32 [8192], P('feat')
- residual: float32 [8192], P('feat')
The draws below stay inside these ranges and needn't reach their ends.
Inputs may be any that keep to these rules, and one draw needn't show every extreme that they name: `labels`: every label is -1 or +1.
All inputs are finite; a program needn't handle non-finite values.
Results may differ from the reference program's by a relative error of at most 0.0003.
Values sent between devices are 32-bit elements; how exact they have to be, the bound alone decides.
A program may use at most 64 MiB of HBM per device.

```python
import jax
import jax.numpy as jnp
from jax import lax

CG_STEPS = 3
SAMPLES = 4096
FEATURES = 8192


def draw_labels(key, part):
    return (2 * jax.random.randint(jax.random.fold_in(key, 11), (SAMPLES,), 0, 2) - 1).astype(jnp.int32)


def steps_of(own_key, shape, cuts, smallest, high):
    def one(axis_at, blocks):
        steps = jax.random.uniform(jax.random.fold_in(jax.random.fold_in(own_key, 6), axis_at), (blocks,), jnp.float32, smallest / len(cuts), high / len(cuts))
        return jnp.repeat(jnp.exp(steps), shape[axis_at] // blocks).reshape((-1,) + (1,) * (len(shape) - axis_at - 1))

    level = one(*cuts[0])
    for cut in cuts[1:]:
        level = level * one(*cut)
    return level


def centred(stream_key, extent, scale, reach, shards=(), dtype=jnp.bfloat16):
    values = jax.random.normal(stream_key, extent, jnp.float32) * scale
    if len(shards) > 0:
        values = steps_of(stream_key, extent, shards, -0.22, 0.18) * values
    return jnp.clip(values, min=-reach, max=reach).astype(dtype)


def setup_inputs(seed: int = 0) -> dict:
    seeds = jax.random.split(jax.random.key(seed), 4)
    return {
        "features": centred(seeds[0], (SAMPLES, FEATURES), FEATURES ** -0.5, 0.0625, ((0, 4), (1, 8)), jnp.float32),
        "labels": draw_labels(jax.random.fold_in(seeds[3], 71), 0),
        "weights": centred(seeds[2], (FEATURES,), 1.0, 6.0, ((0, 8),), jnp.float32),
    }


PENALTY = 4.0


def reference(features, labels, weights):
    hi = lax.Precision.HIGHEST
    y = labels.astype(jnp.float32)
    margin = y * jnp.dot(features, weights, precision=hi)
    sig = 1.0 / (1.0 + jnp.exp(-margin))
    gradient = weights + PENALTY * jnp.dot((sig - 1.0) * y, features, precision=hi)
    curv = PENALTY * sig * (1.0 - sig)
    newton_step = jnp.zeros_like(weights)
    residual = -gradient
    direction = residual
    rr = jnp.sum(residual * residual)
    for step in range(CG_STEPS):
        image = direction + jnp.dot(curv * jnp.dot(features, direction, precision=hi), features, precision=hi)
        alpha = rr / jnp.sum(direction * image)
        newton_step = newton_step + alpha * direction
        residual = residual - alpha * image
        fresh = jnp.sum(residual * residual)
        direction = residual + (fresh / rr) * direction
        rr = fresh
    return gradient, newton_step, residual
```

```python
import functools

import jax
import jax.numpy as jnp
from jax import lax
from jax.experimental import pallas as pl
from jax.experimental.pallas import tpu as pltpu
from jax.sharding import PartitionSpec as P

CG_STEPS = 3
ROUNDS = CG_STEPS + 1
PENALTY = 4.0
MESH = pl.DeviceIdType.MESH
LANES = 128
SUBLANES = 8
CHUNK = 128


def class_order(labels):
    rows = labels.shape[0]
    wide = rows * LANES // SUBLANES
    per = LANES // SUBLANES
    source = labels.astype(jnp.bfloat16)
    lane = lax.broadcasted_iota(jnp.int32, (LANES, wide), 0)
    column = lax.broadcasted_iota(jnp.int32, (LANES, wide), 1)
    row = lax.broadcasted_iota(jnp.int32, (rows, wide), 0)
    keep = row == lax.broadcasted_iota(jnp.int32, (rows, wide), 1) // per
    out = []
    for s in range(SUBLANES):
        pick = (lane == SUBLANES * (column % per) + s).astype(jnp.float32).astype(jnp.bfloat16)
        moved = jnp.dot(source, pick, preferred_element_type=jnp.float32)
        out.append(jnp.sum(jnp.where(keep, moved, 0.0), axis=0, keepdims=True))
    return jnp.concatenate(out, axis=0)


def kernel(nd, nf, x_hbm, labels_ref, weights_ref, grad_ref, newton_ref, resid_ref,
           x, vec, f_out, f_in, fx_out, fx_in, d_out, d_in, dx_out, dx_in,
           load_sem, fs, fr, fxs, fxr, ds, dr, dxs, dxr):
    samples, width = x.shape
    blocks = width // LANES
    chunks = samples // CHUNK
    per = CHUNK // SUBLANES
    my_f, my_d = lax.axis_index("feat"), lax.axis_index("dp")

    loads = []
    for c in range(chunks):
        rows = pl.ds(c * CHUNK, CHUNK)
        load = pltpu.make_async_copy(x_hbm.at[rows], x.at[rows], load_sem.at[c])
        load.start()
        loads.append(load)

    barrier = pltpu.get_barrier_semaphore()
    for k in range(1, nf):
        pl.semaphore_signal(barrier, inc=1, device_id={"feat": lax.rem(my_f + k, nf)}, device_id_type=MESH)
    for k in range(1, nd):
        pl.semaphore_signal(barrier, inc=1, device_id={"dp": lax.rem(my_d + k, nd)}, device_id_type=MESH)

    pending = []

    def publish(axis, me, n, out, inbox, send, recv, value, step):
        out[step] = value
        inbox[step, me] = value
        for k in range(n - 1, 0, -1):
            copy = pltpu.make_async_remote_copy(
                src_ref=out.at[step],
                dst_ref=inbox.at[step, me],
                send_sem=send.at[step, k],
                recv_sem=recv.at[step, me],
                device_id={axis: lax.rem(me + k, n)},
                device_id_type=MESH,
            )
            copy.start()
            pending.append(copy)

    def collect(axis, me, n, out, inbox, send, recv, step):
        for k in range(1, n):
            peer = lax.rem(me + k, n)
            pltpu.make_async_remote_copy(
                src_ref=out.at[step],
                dst_ref=inbox.at[step, peer],
                send_sem=send.at[step, k],
                recv_sem=recv.at[step, peer],
                device_id={axis: peer},
                device_id_type=MESH,
            ).wait_recv()
        parts = [inbox[step, i] for i in range(n)]
        while len(parts) > 1:
            parts = [sum(parts[i + 1 : i + 2], parts[i]) for i in range(0, len(parts), 2)]
        return parts[0]

    feat = ("feat", my_f, nf, f_out, f_in, fs, fr)
    feat_x = ("feat", my_f, nf, fx_out, fx_in, fxs, fxr)
    dp = ("dp", my_d, nd, d_out, d_in, ds, dr)
    dp_x = ("dp", my_d, nd, dx_out, dx_in, dxs, dxr)

    lane = lax.broadcasted_iota(jnp.int32, (SUBLANES, samples // SUBLANES), 1)

    def forward(v, first=False):
        total = jnp.zeros((SUBLANES, samples // SUBLANES), jnp.float32)
        rows_of = [jnp.broadcast_to(v[k : k + 1, :], (CHUNK, LANES)) for k in range(blocks)]
        for c in range(chunks):
            if first:
                loads[c].wait()
            part = None
            for k in range(blocks):
                term = x[c * CHUNK : (c + 1) * CHUNK, k * LANES : (k + 1) * LANES] * rows_of[k]
                part = term if part is None else part + term
            sums = jnp.sum(part, axis=1, keepdims=True)
            for j in range(per):
                piece = jnp.broadcast_to(sums[j * SUBLANES : (j + 1) * SUBLANES], total.shape)
                total = jnp.where(lane == c * per + j, piece, total)
        return total

    def backward(u):
        acc = [jnp.zeros((SUBLANES, LANES), jnp.float32)] * blocks
        for c in range(chunks):
            wide = [
                jnp.broadcast_to(u[:, c * per + j : c * per + j + 1], (SUBLANES, LANES)) for j in range(per)
            ]
            for k in range(blocks):
                for j in range(per):
                    top = c * CHUNK + j * SUBLANES
                    acc[k] = acc[k] + x[top : top + SUBLANES, k * LANES : (k + 1) * LANES] * wide[j]
        return jnp.concatenate([jnp.sum(a, axis=0, keepdims=True) for a in acc], axis=0)

    def whole(row):
        return jnp.sum(row, axis=1, keepdims=True)

    def fold(a):
        return jnp.sum(a, axis=0, keepdims=True)

    weights = weights_ref[...]
    margin_part = forward(weights, first=True)
    pl.semaphore_wait(barrier, nf - 1 + nd - 1)
    publish(*feat, margin_part, 0)
    y = class_order(labels_ref[...])
    margin = y * collect(*feat, 0)
    sig = 1.0 / (1.0 + jnp.exp(-margin))
    publish(*dp, backward((sig - 1.0) * y), 0)
    curv = PENALTY * sig * (1.0 - sig)
    gradient = weights + PENALTY * collect(*dp, 0)
    grad_ref[...] = gradient

    residual = -gradient
    direction = residual
    newton = jnp.zeros_like(gradient)
    rr = dir_sq = image_rows = None
    for step in range(1, ROUNDS):
        squares = fold(residual * residual)
        cross = fold(residual * direction)
        publish(*feat_x, jnp.concatenate([squares, cross], axis=0), step - 1)
        publish(*feat, forward(residual), step)
        sums = collect(*feat_x, step - 1)
        fresh = whole(sums[0:1])
        mixed = whole(sums[1:2])
        res_rows = collect(*feat, step)
        if step == 1:
            dir_sq, image_rows = fresh, res_rows
        else:
            beta = fresh / rr
            direction = residual + beta * direction
            image_rows = res_rows + beta * image_rows
            dir_sq = fresh + beta * (2.0 * mixed + beta * dir_sq)
        rr = fresh
        weighted = curv * image_rows
        publish(*dp_x, fold(weighted * image_rows), step - 1)
        publish(*dp, backward(weighted), step)
        quad = whole(collect(*dp_x, step - 1))
        alpha = rr / (dir_sq + quad)
        back = collect(*dp, step)
        newton = newton + alpha * direction
        residual = residual - alpha * (direction + back)
    newton_ref[...] = newton
    resid_ref[...] = residual
    for copy in pending:
        copy.wait_send()


def solution(mesh):
    nd, nf = mesh.shape["dp"], mesh.shape["feat"]
    placed = (P("dp", "feat"), P("dp"), P("feat"))

    def local(features, labels, weights):
        samples, width = features.shape
        blocks = width // LANES
        compact = (SUBLANES, samples // SUBLANES)
        rows = (blocks, LANES)
        f32 = jnp.float32
        dma = pltpu.SemaphoreType.DMA
        vmem = pl.BlockSpec(memory_space=pltpu.VMEM)
        outs = pl.pallas_call(
            functools.partial(kernel, nd, nf),
            out_shape=[jax.ShapeDtypeStruct(rows, f32)] * 3,
            in_specs=[pl.BlockSpec(memory_space=pl.ANY), vmem, vmem],
            out_specs=[vmem] * 3,
            scratch_shapes=[
                pltpu.VMEM((samples, width), f32),
                pltpu.VMEM(rows, f32),
                pltpu.VMEM((ROUNDS,) + compact, f32),
                pltpu.VMEM((ROUNDS, nf) + compact, f32),
                pltpu.VMEM((CG_STEPS, 2, LANES), f32),
                pltpu.VMEM((CG_STEPS, nf, 2, LANES), f32),
                pltpu.VMEM((ROUNDS,) + rows, f32),
                pltpu.VMEM((ROUNDS, nd) + rows, f32),
                pltpu.VMEM((CG_STEPS, 1, samples // SUBLANES), f32),
                pltpu.VMEM((CG_STEPS, nd, 1, samples // SUBLANES), f32),
                dma((samples // CHUNK,)),
                dma((ROUNDS, nf)),
                dma((ROUNDS, nf)),
                dma((CG_STEPS, nf)),
                dma((CG_STEPS, nf)),
                dma((ROUNDS, nd)),
                dma((ROUNDS, nd)),
                dma((CG_STEPS, nd)),
                dma((CG_STEPS, nd)),
            ],
            compiler_params=pltpu.CompilerParams(
                collective_id=0, has_side_effects=True, vmem_limit_bytes=60 * 1024 * 1024
            ),
        )(features, labels.reshape(samples // LANES, LANES), weights.reshape(rows))
        return tuple(out.reshape(width) for out in outs)

    return jax.shard_map(
        local,
        mesh=mesh,
        in_specs=placed,
        out_specs=(P("feat"), P("feat"), P("feat")),
        check_vma=False,
    )
```

```python
import functools

import jax
import jax.numpy as jnp
from jax import lax
from jax.experimental import pallas as pl
from jax.experimental.pallas import tpu as pltpu
from jax.sharding import PartitionSpec as P

CG_STEPS = 3
ROUNDS = CG_STEPS + 1
PENALTY = 4.0
MESH = pl.DeviceIdType.MESH
LANES = 128
SUBLANES = 8
CHUNK = 128


def class_order(labels):
    rows = labels.shape[0]
    wide = rows * LANES // SUBLANES
    per = LANES // SUBLANES
    source = labels.astype(jnp.bfloat16)
    lane = lax.broadcasted_iota(jnp.int32, (LANES, wide), 0)
    column = lax.broadcasted_iota(jnp.int32, (LANES, wide), 1)
    row = lax.broadcasted_iota(jnp.int32, (rows, wide), 0)
    keep = row == lax.broadcasted_iota(jnp.int32, (rows, wide), 1) // per
    out = []
    for s in range(SUBLANES):
        pick = (lane == SUBLANES * (column % per) + s).astype(jnp.float32).astype(jnp.bfloat16)
        moved = jnp.dot(source, pick, preferred_element_type=jnp.float32)
        out.append(jnp.sum(jnp.where(keep, moved, 0.0), axis=0, keepdims=True))
    return jnp.concatenate(out, axis=0)


def kernel(nd, nf, x_hbm, labels_ref, weights_ref, out_ref,
           x, vec, f_out, f_in, fx_out, fx_in, d_out, d_in, dx_out, dx_in,
           load_sem, fs, fr, fxs, fxr, ds, dr, dxs, dxr):
    samples, width = x.shape
    blocks = width // LANES
    chunks = samples // CHUNK
    per = CHUNK // SUBLANES
    my_f, my_d = lax.axis_index("feat"), lax.axis_index("dp")

    loads = []
    for c in range(chunks):
        rows = pl.ds(c * CHUNK, CHUNK)
        load = pltpu.make_async_copy(x_hbm.at[rows], x.at[rows], load_sem.at[c])
        load.start()
        loads.append(load)

    barrier = pltpu.get_barrier_semaphore()
    for k in range(1, nf):
        pl.semaphore_signal(barrier, inc=1, device_id={"feat": lax.rem(my_f + k, nf)}, device_id_type=MESH)
    for k in range(1, nd):
        pl.semaphore_signal(barrier, inc=1, device_id={"dp": lax.rem(my_d + k, nd)}, device_id_type=MESH)

    pending = []

    def publish(axis, me, n, out, inbox, send, recv, value, step):
        out[step] = value
        inbox[step, me] = value
        for k in range(n - 1, 0, -1):
            copy = pltpu.make_async_remote_copy(
                src_ref=out.at[step],
                dst_ref=inbox.at[step, me],
                send_sem=send.at[step, k],
                recv_sem=recv.at[step, me],
                device_id={axis: lax.rem(me + k, n)},
                device_id_type=MESH,
            )
            copy.start()
            pending.append(copy)

    def collect(axis, me, n, out, inbox, send, recv, step):
        for k in range(1, n):
            peer = lax.rem(me + k, n)
            pltpu.make_async_remote_copy(
                src_ref=out.at[step],
                dst_ref=inbox.at[step, peer],
                send_sem=send.at[step, k],
                recv_sem=recv.at[step, peer],
                device_id={axis: peer},
                device_id_type=MESH,
            ).wait_recv()
        parts = [inbox[step, i] for i in range(n)]
        while len(parts) > 1:
            parts = [sum(parts[i + 1 : i + 2], parts[i]) for i in range(0, len(parts), 2)]
        return parts[0]

    feat = ("feat", my_f, nf, f_out, f_in, fs, fr)
    feat_x = ("feat", my_f, nf, fx_out, fx_in, fxs, fxr)
    dp = ("dp", my_d, nd, d_out, d_in, ds, dr)
    dp_x = ("dp", my_d, nd, dx_out, dx_in, dxs, dxr)

    lane = lax.broadcasted_iota(jnp.int32, (SUBLANES, samples // SUBLANES), 1)

    def forward(v, first=False):
        total = jnp.zeros((SUBLANES, samples // SUBLANES), jnp.float32)
        rows_of = [jnp.broadcast_to(v[k : k + 1, :], (CHUNK, LANES)) for k in range(blocks)]
        for c in range(chunks):
            if first:
                loads[c].wait()
            part = None
            for k in range(blocks):
                term = x[c * CHUNK : (c + 1) * CHUNK, k * LANES : (k + 1) * LANES] * rows_of[k]
                part = term if part is None else part + term
            sums = jnp.sum(part, axis=1, keepdims=True)
            for j in range(per):
                piece = jnp.broadcast_to(sums[j * SUBLANES : (j + 1) * SUBLANES], total.shape)
                total = jnp.where(lane == c * per + j, piece, total)
        return total

    def backward(u):
        acc = [jnp.zeros((SUBLANES, LANES), jnp.float32)] * blocks
        for c in range(chunks):
            wide = [
                jnp.broadcast_to(u[:, c * per + j : c * per + j + 1], (SUBLANES, LANES)) for j in range(per)
            ]
            for k in range(blocks):
                for j in range(per):
                    top = c * CHUNK + j * SUBLANES
                    acc[k] = acc[k] + x[top : top + SUBLANES, k * LANES : (k + 1) * LANES] * wide[j]
        return jnp.concatenate([jnp.sum(a, axis=0, keepdims=True) for a in acc], axis=0)

    def whole(row):
        return jnp.sum(row, axis=1, keepdims=True)

    def fold(a):
        return jnp.sum(a, axis=0, keepdims=True)

    weights = weights_ref[...]
    margin_part = forward(weights, first=True)
    pl.semaphore_wait(barrier, nf - 1 + nd - 1)
    publish(*feat, margin_part, 0)
    y = class_order(labels_ref[...])
    margin = y * collect(*feat, 0)
    sig = 1.0 / (1.0 + jnp.exp(-margin))
    publish(*dp, backward((sig - 1.0) * y), 0)
    curv = PENALTY * sig * (1.0 - sig)
    gradient = weights + PENALTY * collect(*dp, 0)
    out_ref[0] = gradient

    residual = -gradient
    direction = residual
    newton = jnp.zeros_like(gradient)
    rr = dir_sq = image_rows = None
    for step in range(1, ROUNDS):
        squares = fold(residual * residual)
        cross = fold(residual * direction)
        publish(*feat_x, jnp.concatenate([squares, cross], axis=0), step - 1)
        publish(*feat, forward(residual), step)
        sums = collect(*feat_x, step - 1)
        fresh = whole(sums[0:1])
        mixed = whole(sums[1:2])
        res_rows = collect(*feat, step)
        if step == 1:
            dir_sq, image_rows = fresh, res_rows
        else:
            beta = fresh / rr
            direction = residual + beta * direction
            image_rows = res_rows + beta * image_rows
            dir_sq = fresh + beta * (2.0 * mixed + beta * dir_sq)
        rr = fresh
        weighted = curv * image_rows
        publish(*dp_x, fold(weighted * image_rows), step - 1)
        publish(*dp, backward(weighted), step)
        quad = whole(collect(*dp_x, step - 1))
        alpha = rr / (dir_sq + quad)
        back = collect(*dp, step)
        newton = newton + alpha * direction
        residual = residual - alpha * (direction + back)
    out_ref[1] = newton
    out_ref[2] = residual
    for copy in pending:
        copy.wait_send()


def solution(mesh):
    nd, nf = mesh.shape["dp"], mesh.shape["feat"]
    placed = (P("dp", "feat"), P("dp"), P("feat"))

    def local(features, labels, weights):
        samples, width = features.shape
        blocks = width // LANES
        compact = (SUBLANES, samples // SUBLANES)
        rows = (blocks, LANES)
        f32 = jnp.float32
        dma = pltpu.SemaphoreType.DMA
        vmem = pl.BlockSpec(memory_space=pltpu.VMEM)
        outs = pl.pallas_call(
            functools.partial(kernel, nd, nf),
            out_shape=jax.ShapeDtypeStruct((3,)+rows, f32),
            in_specs=[pl.BlockSpec(memory_space=pl.ANY), vmem, vmem],
            out_specs=vmem,
            scratch_shapes=[
                pltpu.VMEM((samples, width), f32),
                pltpu.VMEM(rows, f32),
                pltpu.VMEM((ROUNDS,) + compact, f32),
                pltpu.VMEM((ROUNDS, nf) + compact, f32),
                pltpu.VMEM((CG_STEPS, 2, LANES), f32),
                pltpu.VMEM((CG_STEPS, nf, 2, LANES), f32),
                pltpu.VMEM((ROUNDS,) + rows, f32),
                pltpu.VMEM((ROUNDS, nd) + rows, f32),
                pltpu.VMEM((CG_STEPS, 1, samples // SUBLANES), f32),
                pltpu.VMEM((CG_STEPS, nd, 1, samples // SUBLANES), f32),
                dma((samples // CHUNK,)),
                dma((ROUNDS, nf)),
                dma((ROUNDS, nf)),
                dma((CG_STEPS, nf)),
                dma((CG_STEPS, nf)),
                dma((ROUNDS, nd)),
                dma((ROUNDS, nd)),
                dma((CG_STEPS, nd)),
                dma((CG_STEPS, nd)),
            ],
            compiler_params=pltpu.CompilerParams(
                collective_id=0, has_side_effects=True, vmem_limit_bytes=60 * 1024 * 1024
            ),
        )(features, labels.reshape(samples // LANES, LANES), weights.reshape(rows))
        return tuple(outs[i].reshape(width) for i in range(3))

    return jax.shard_map(
        local,
        mesh=mesh,
        in_specs=placed,
        out_specs=(P("feat"), P("feat"), P("feat")),
        check_vma=False,
    )
```
